32 devices in a mesh: col: 32 (over z, y, x, core).
Axes of the slice: x: 2, y: 2, z: 4, core: 2. Of those that a mesh axis runs over, the one named last changes fastest.
Arguments:
- matrix: float32 [4096, 4096], P(None, 'col'), as said below
- rhs_rows: float32 [2048, 4096], P('col'), may hold values from -6 to 6
Outputs:
- eliminated: float32 [4096, 4096], P(None, 'col')
- solved_rows: float32 [2048, 4096], P('col')
The draws below stay inside these ranges and needn't reach their ends.
Inputs may be any that keep to these rules, and one draw needn't show every extreme that they name: `matrix`: the diagonal entries lie between 1.5 * sqrt(4096) and 3 * sqrt(4096); the other entries between -4 and 4.
All inputs are finite; a program needn't handle non-finite values.
Results may differ from the reference program's by a relative error of at most 0.0001.
Values sent between devices are 32-bit elements; how exact they have to be, the bound alone decides.
No kernel may reach another device: no remote copies, remote signals or barrier semaphores. Data moves between devices by JAX's collectives and lax.ppermute only.
A program may use at most 192 MiB of HBM per device.

```python
import math
import jax
import jax.numpy as jnp
from jax import lax

BLK = 128
BLK_DEV = 1
STEPS = 2
NMAT = 4096
RHS = 2048


def draw_matrix(key, part):
    first_key, second_key = jax.random.split(jax.random.fold_in(key, 17))
    spread = jnp.clip(jax.random.normal(first_key, (NMAT, NMAT), jnp.float32), -4.0, 4.0)
    root_order = math.sqrt(NMAT)
    diag_values = jax.random.uniform(second_key, (NMAT,), jnp.float32, 1.5 * root_order, 3.0 * root_order)
    positions = jnp.arange(NMAT)
    return spread.at[positions, positions].set(diag_values)


def shard_levels(rng, extent, cuts, smallest, largest):
    def one(axis_at, shards_of):
        steps = jax.random.uniform(jax.random.fold_in(jax.random.fold_in(rng, 6), axis_at), (shards_of,), jnp.float32, smallest / len(cuts), largest / len(cuts))
        return jnp.repeat(jnp.exp(steps), extent[axis_at] // shards_of).reshape((-1,) + (1,) * (len(extent) - axis_at - 1))

    factor_of = one(*cuts[0])
    for cut in cuts[1:]:
        factor_of = factor_of * one(*cut)
    return factor_of


def centred(rng, dims, width, bound, cuts=(), held_as=jnp.bfloat16):
    values = width * jax.random.normal(rng, dims, jnp.float32)
    if cuts:
        values = values * shard_levels(rng, dims, cuts, -0.22, 0.18)
    return jnp.clip(values, -bound, bound).astype(held_as)


def setup_inputs(seed: int = 0) -> dict:
    streams_of = jax.random.split(jax.random.key(seed), 3)
    return {
        "matrix": draw_matrix(jax.random.fold_in(streams_of[2], 71), 0),
        "rhs_rows": centred(streams_of[1], (RHS, NMAT), 1.0, 6.0, ((0, 32),), jnp.float32),
    }


def pivot_inverse(pivot_block):
    gram = jnp.dot(pivot_block.T.astype(jnp.float32), pivot_block.astype(jnp.float32), precision=lax.Precision.HIGHEST, preferred_element_type=jnp.float32)
    lower = jnp.linalg.cholesky(gram)
    return jax.scipy.linalg.cho_solve((lower, True), pivot_block.T)

def reference(matrix, rhs_rows):
    precise = lax.Precision.HIGHEST
    for step in range(STEPS):
        row_start = step * BLK_DEV * BLK
        row_end = row_start + BLK
        panel_cols = matrix[:, row_start:row_end]
        inverse = pivot_inverse(panel_cols[row_start:row_end])
        scaled = jnp.dot(inverse.astype(jnp.float32), matrix[row_start:row_end].astype(jnp.float32), precision=precise, preferred_element_type=jnp.float32)
        matrix = matrix - jnp.dot(panel_cols.astype(jnp.float32), scaled.astype(jnp.float32), precision=precise, preferred_element_type=jnp.float32)
        matrix = matrix.at[row_start:row_end].set(scaled)
        column = -jnp.dot(panel_cols.astype(jnp.float32), inverse.astype(jnp.float32), precision=precise, preferred_element_type=jnp.float32)
        column = column.at[row_start:row_end].set(inverse)
        matrix = matrix.at[:, row_start:row_end].set(column)
        solved = jnp.dot(rhs_rows[:, row_start:row_end].astype(jnp.float32), inverse.T.astype(jnp.float32), precision=precise, preferred_element_type=jnp.float32)
        rhs_rows = rhs_rows - jnp.dot(solved.astype(jnp.float32), panel_cols.T.astype(jnp.float32), precision=precise, preferred_element_type=jnp.float32)
        rhs_rows = rhs_rows.at[:, row_start:row_end].set(solved)
    return (matrix, rhs_rows)
```

```python
import functools

import jax
import jax.numpy as jnp
from jax import lax
from jax.experimental import pallas as pl
from jax.experimental.pallas import tpu as pltpu
from jax.sharding import PartitionSpec as P

STEPS = 2
CORES = 2


def dot(a, b, dims=((1,), (0,))):
    return lax.dot_general(
        a, b, (dims, ((), ())), precision=lax.Precision.HIGHEST, preferred_element_type=jnp.float32
    )


def split(value):
    high = value.astype(jnp.bfloat16)
    return high, (value - high.astype(jnp.float32)).astype(jnp.bfloat16)


def inverse_kernel(flag_ref, block_ref, out_ref, x_ref, e_ref):
    order = block_ref.shape[0]

    @pl.when(flag_ref[0] == 0)
    def _():
        out_ref[...] = jnp.zeros_like(out_ref)

    @pl.when(flag_ref[0] != 0)
    def _():
        rows = lax.broadcasted_iota(jnp.int32, (order, order), 0)
        cols = lax.broadcasted_iota(jnp.int32, (order, order), 1)
        unit = jnp.where(rows == cols, 1.0, 0.0).astype(jnp.float32)

        def residual():
            left = unit - dot(block_ref[...], x_ref[...])
            e_ref[...] = left
            return jnp.sum(left * left)

        diag = block_ref[...] * unit
        by_row = 1.0 / jnp.sum(diag, axis=1, keepdims=True)
        by_col = 1.0 / jnp.sum(diag, axis=0, keepdims=True)
        x_ref[...] = by_row * (2.0 * unit - block_ref[...] * by_col)
        first = residual()
        good = first < 0.5

        @pl.when(jnp.logical_not(good))
        def _():
            size = jnp.abs(block_ref[...])
            bound = jnp.max(jnp.sum(size, axis=0)) * jnp.max(jnp.sum(size, axis=1))
            x_ref[...] = block_ref[...].T / bound

        start = lax.cond(good, lambda: first, residual)

        def unfinished(state):
            step, now, done = state
            return jnp.logical_and(step < 80, jnp.logical_not(done))

        def advance(state):
            step, now, done = state
            x_ref[...] = x_ref[...] + dot(x_ref[...], e_ref[...])
            fine = now < 1e-7

            def again():
                return residual()

            later = lax.cond(fine, lambda: 0.0, again)
            stalled = jnp.logical_and(now < 0.5, later > 0.5 * now)
            return step + 1, later, jnp.logical_or(fine, stalled)

        lax.while_loop(unfinished, advance, (0, start, False))
        out_ref[...] = x_ref[...]


def pivot_inverse(flag, block):
    order = block.shape[0]
    return pl.pallas_call(
        inverse_kernel,
        out_shape=jax.ShapeDtypeStruct((order, order), jnp.float32),
        in_specs=[
            pl.BlockSpec(memory_space=pltpu.SMEM),
            pl.BlockSpec(memory_space=pltpu.VMEM),
        ],
        out_specs=pl.BlockSpec(memory_space=pltpu.VMEM),
        scratch_shapes=[pltpu.VMEM((order, order), jnp.float32)] * 2,
        name="pivot_inverse",
    )(flag, block)


def update_kernel(
    info_ref, inv_own_ref, inv_par_ref, own_ref, par_ref, top_ref, m_ref, rtop_ref, r_ref,
    m_out, r_out, high_ref, low_ref,
):
    block = pl.program_id(0)
    wide = own_ref.shape[-1]
    core, pivot = info_ref[0], info_ref[1] == 0

    def ordered(own, par, axis):
        return jnp.where(
            core == 0,
            jnp.concatenate([own, par], axis),
            jnp.concatenate([par, own], axis),
        )

    @pl.when(block == 0)
    def _():
        inverse = ordered(inv_own_ref[0], inv_par_ref[0], 1)
        rows = lax.broadcasted_iota(jnp.int32, top_ref.shape, 0)
        cols = lax.broadcasted_iota(jnp.int32, top_ref.shape, 1) + core * wide
        unit = jnp.where(rows == cols, 1.0, 0.0).astype(jnp.float32)
        scaled = dot(inverse, jnp.where(pivot, unit, top_ref[...]))
        solved = dot(rtop_ref[...], inverse, ((1,), (1,)))
        m_out[...] = scaled
        r_out[...] = solved
        both = jnp.concatenate([scaled, solved.T], 1)
        both = ordered(both[:wide], both[wide:], 0)
        high, low = split(both)
        high_ref[...] = high
        low_ref[...] = low

    @pl.when(block != 0)
    def _():
        panel = jnp.concatenate([own_ref[0], par_ref[0]], 1)
        high, low = split(panel)
        mul = functools.partial(jnp.dot, preferred_element_type=jnp.float32)
        gone = mul(high, high_ref[...]) + (mul(high, low_ref[...]) + mul(low, high_ref[...]))
        m_out[...] = jnp.where(pivot, 0.0, m_ref[...]) - gone[:, :wide]
        r_out[...] = r_ref[...] - gone[:, wide:].T


def update(info, own, par, matrix, rhs_rows):
    pieces, depth, wide = own.shape
    rows = rhs_rows.shape[0]

    def own_at(j, info):
        return info[2 + j], 0, 0

    def par_at(j, info):
        return info[2 + pieces + j], 0, 0

    spec = pl.BlockSpec
    return pl.pallas_call(
        update_kernel,
        out_shape=(
            jax.ShapeDtypeStruct(matrix.shape, jnp.float32),
            jax.ShapeDtypeStruct(rhs_rows.shape, jnp.float32),
        ),
        grid_spec=pltpu.PrefetchScalarGridSpec(
            num_scalar_prefetch=1,
            grid=(pieces,),
            in_specs=[
                spec((1, depth, wide), lambda j, info: own_at(0, info)),
                spec((1, depth, wide), lambda j, info: par_at(0, info)),
                spec((1, depth, wide), own_at),
                spec((1, depth, wide), par_at),
                spec((depth, wide), lambda j, info: (0, 0)),
                spec((depth, wide), lambda j, info: (j, 0)),
                spec((rows, depth), lambda j, info: (0, 0)),
                spec((rows, depth), lambda j, info: (0, j)),
            ],
            out_specs=[
                spec((depth, wide), lambda j, info: (j, 0)),
                spec((rows, depth), lambda j, info: (0, j)),
            ],
            scratch_shapes=[pltpu.VMEM((depth, wide + rows), jnp.bfloat16)] * 2,
        ),
        name="update",
    )(info, own, par, own, par, matrix, matrix, rhs_rows, rhs_rows)


def body(chips, matrix, rhs_rows):
    depth = matrix.shape[0] // chips
    bits = chips.bit_length() - 1
    assert chips == 1 << bits and depth == STEPS * matrix.shape[1]
    order = [[], []]
    for pair in range((bits + 1) // 2):
        a, b = bits - 1 - pair, pair
        order[0] += [a, b] if a != b else [a]
        order[1] += [b, a] if a != b else [a]

    me = lax.axis_index("col")
    chip, core = me // CORES, me % CORES
    root, first = chip == 0, core == 0

    def send(value, pairs):
        return lax.ppermute(value, "col", pairs)

    def piece(k):
        return matrix[k * depth:(k + 1) * depth]

    swap = [(i, i ^ 1) for i in range(CORES * chips)]

    far = 1 << order[1][0]
    sums = [0.0, 0.0]
    for k in range(1, chips):
        near = k & ~far
        pairs = [(0, CORES * k)] + ([(1, CORES * near + 1)] if near else [])
        got = send(piece(k), pairs)
        sums[(k & far) != 0] += got

    top = piece(0)
    other = send(top, swap)
    block = jnp.where(
        first, jnp.concatenate([top, other], 1), jnp.concatenate([other, top], 1)
    )
    inverse = pivot_inverse(root.astype(jnp.int32)[None], block)
    half = jnp.where(first, inverse[:, :top.shape[1]], inverse[:, top.shape[1]:])

    even = jnp.where(root, half, sums[0])
    odd = jnp.where(root & ~first, piece(far), sums[1])
    whole = [(CORES * c, CORES * (c ^ (1 << order[0][0]))) for c in range(chips)]
    down = [(CORES * c + 1, CORES * (c | far) + 1) for c in range(chips) if not c & far]
    one = send(jnp.where(first, even + odd, even), whole + down)
    two = send(odd, down)
    stack = jnp.stack([even + jnp.where(first, odd, two), one + jnp.where(first, 0.0, odd)])
    for level in range(1, bits):
        pairs = [
            (CORES * c + p, CORES * (c ^ (1 << order[p][level])) + p)
            for c in range(chips)
            for p in range(CORES)
        ]
        stack = jnp.concatenate([stack, send(stack, pairs)])
    partner = send(stack, swap)

    def place(p):
        away = jnp.arange(chips, dtype=jnp.int32) ^ chip
        return sum(((away >> bit) & 1) << level for level, bit in enumerate(order[p]))

    mine, theirs = place(0), place(1)
    info = jnp.concatenate([
        jnp.stack([core, chip]).astype(jnp.int32),
        jnp.where(first, mine, theirs),
        jnp.where(first, theirs, mine),
    ])
    return tuple(update(info, stack, partner, matrix, rhs_rows))


def solution(mesh):
    chips = mesh.shape["col"] // CORES
    return jax.shard_map(
        functools.partial(body, chips),
        mesh=mesh,
        in_specs=(P(None, "col"), P("col", None)),
        out_specs=(P(None, "col"), P("col", None)),
        check_vma=False,
    )
```
